32 devices in a mesh: fsdp: 4 (over y, x), tenant: 4 (over z), dp: 2 (over core).
Axes of the slice: x: 2, y: 2, z: 4, core: 2. Of those that a mesh axis runs over, the one named last changes fastest.
Arguments:
- tokens: bfloat16 [3072, 5120], P(('fsdp', 'dp'), 'tenant'), may hold values from -6 to 6
- block_tenant_index: int32 [48], P(('fsdp', 'dp')), may hold values from 0 to 7
- ranks: int32 [8], replicated, may hold values from 16 to 64, as said below
- frozen_up_weight: bfloat16 [5120, 14336], P(('fsdp', 'dp'), 'tenant'), may hold values from -0.078125 to 0.078125
- tenant_down_adapters: bfloat16 [8, 64, 5120], P('tenant'), may hold values from -0.078125 to 0.078125
- tenant_up_adapters: bfloat16 [8, 64, 14336], P('tenant'), may hold values from -0.75 to 0.75
- cotangent: bfloat16 [3072, 14336], P(('fsdp', 'dp'), 'tenant'), may hold values from -6 to 6
Outputs:
- hidden_out: bfloat16 [3072, 14336], P(('fsdp', 'dp'), 'tenant')
- grad_tokens: bfloat16 [3072, 5120], P(('fsdp', 'dp'), 'tenant')
- grad_down: float32 [8, 64, 5120], P('dp', None, 'tenant')
- grad_up: float32 [8, 64, 14336], P('dp', None, 'tenant')
The draws below stay inside these ranges and needn't reach their ends.
Inputs may be any that keep to these rules, and one draw needn't show every extreme that they name: `ranks`: multiples of 16; some tenant has rank 64.
All inputs are finite; a program needn't handle non-finite values.
Results may differ from the reference program's by a relative error of at most 0.0034.
Values may be sent and summed in bfloat16 or wider, within the bound.
A program may use at most 128 MiB of HBM per device.

```python
import math
import jax
import jax.numpy as jnp
import numpy as np

MODEL_WIDTH = 5120
HIDDEN_UNITS = 14336
TENANT_COUNT = 8
ADAPTER_RANK = 64
BLOCK = 64
TOKENS = 3072
BLOCKS = 48


def draw_ranks(key, part):
    levels = jax.random.randint(key, (TENANT_COUNT,), 1, ADAPTER_RANK // 16 + 1)
    chosen = jax.random.randint(jax.random.fold_in(key, 7), (), 0, TENANT_COUNT)
    levels = jnp.where(jnp.arange(TENANT_COUNT) == chosen, ADAPTER_RANK // 16, levels)
    return (levels * 16).astype(jnp.int32)


def place_ends(drawn, key, least, high):
    place = [jax.random.randint(jax.random.fold_in(key, axis), (), 0, length) for axis, length in enumerate(drawn.shape)]
    main_axis = drawn.shape.index(max(drawn.shape))
    next_to = place[:main_axis] + [(place[main_axis] + 1) % drawn.shape[main_axis]] + place[main_axis + 1:]
    return drawn.at[tuple(place)].set(least).at[tuple(next_to)].set(high)


def shard_levels(key, extent, shards, smallest, top_value):
    factor_of = 1.0
    for dim, blocks in shards:
        steps = jax.random.uniform(jax.random.fold_in(jax.random.fold_in(key, 6), dim), (blocks,), jnp.float32, smallest / len(shards), top_value / len(shards))
        factor_of = factor_of * jnp.repeat(jnp.exp(steps), extent[dim] // blocks).reshape((-1,) + (1,) * (len(extent) - 1 - dim))
    return factor_of


def rank_table(number_of, lean):
    weights = [(1 << 20) // math.isqrt(grade ** lean) + 1 for grade in range(1, number_of + 1)]
    deviation = 1 + sum(weights) // (1 << 30)
    return np.cumsum(np.array([max(1, weight // deviation) for weight in weights]))


def ranked(stream_key, extent, number_of, skew):
    grid = rank_table(number_of, skew)
    pick = jax.random.randint(jax.random.fold_in(stream_key, 1), extent, 0, int(grid[number_of - 1]))
    rank = jnp.searchsorted(jnp.asarray(grid, jnp.int32), pick, side="right")
    return jax.random.permutation(jax.random.fold_in(stream_key, 2), number_of)[rank].astype(jnp.int32)


def centred(stream_key, extent, spread, most, shards=(), kind=jnp.bfloat16):
    result = spread * jax.random.normal(stream_key, extent, jnp.float32)
    if shards:
        result = result * shard_levels(stream_key, extent, shards, -0.22, 0.18)
    return jnp.clip(result, -most, most).astype(kind)


def setup_inputs(seed: int = 0) -> dict:
    splits = jax.random.split(jax.random.key(seed), 8)
    return {
        "tokens": centred(splits[0], (TOKENS, MODEL_WIDTH), 1.0, 6.0, ((0, 8), (1, 4))),
        "block_tenant_index": place_ends(ranked(splits[1], (BLOCKS,), TENANT_COUNT, 2), jax.random.fold_in(splits[1], 3), 0, TENANT_COUNT - 1).astype(jnp.int32),
        "ranks": draw_ranks(jax.random.fold_in(splits[7], 71), 0),
        "frozen_up_weight": centred(splits[3], (MODEL_WIDTH, HIDDEN_UNITS), MODEL_WIDTH ** -0.5, 0.078125, ((0, 8), (1, 4))),
        "tenant_down_adapters": centred(splits[4], (TENANT_COUNT, ADAPTER_RANK, MODEL_WIDTH), MODEL_WIDTH ** -0.5, 0.078125, ((0, 4),)),
        "tenant_up_adapters": centred(splits[5], (TENANT_COUNT, ADAPTER_RANK, HIDDEN_UNITS), ADAPTER_RANK ** -0.5, 0.75, ((0, 4),)),
        "cotangent": centred(splits[6], (TOKENS, HIDDEN_UNITS), 1.0, 6.0, ((0, 8), (1, 4))),
    }


alpha_scale = 32.0


def make_gain(block_tenant_index, ranks):
    rows_tenant = jnp.repeat(block_tenant_index, BLOCK, total_repeat_length=TOKENS)
    columns = jnp.arange(TENANT_COUNT * ADAPTER_RANK, dtype=jnp.int32)
    col_tenant = columns // ADAPTER_RANK
    col_slot = columns % ADAPTER_RANK
    ranks_col = jnp.repeat(ranks, ADAPTER_RANK, total_repeat_length=TENANT_COUNT * ADAPTER_RANK)
    keep = (rows_tenant[:, None] == col_tenant[None, :]) & (col_slot[None, :] < ranks_col[None, :])
    scale_col = alpha_scale / ranks_col.astype(jnp.float32)
    return jnp.where(keep, scale_col[None, :], jnp.float32(0.0))


def reference(tokens, block_tenant_index, ranks, frozen_up_weight, tenant_down_adapters, tenant_up_adapters, cotangent):
    gain = make_gain(block_tenant_index, ranks)
    flattened_down = tenant_down_adapters.reshape(TENANT_COUNT * ADAPTER_RANK, MODEL_WIDTH)
    flattened_up = tenant_up_adapters.reshape(TENANT_COUNT * ADAPTER_RANK, HIDDEN_UNITS)
    proj = jnp.dot(tokens, flattened_down.T, preferred_element_type=jnp.float32)
    adapted = (proj * gain).astype(jnp.bfloat16)
    base = jnp.dot(tokens, frozen_up_weight, preferred_element_type=jnp.float32)
    hidden_out = (base + jnp.dot(adapted, flattened_up, preferred_element_type=jnp.float32)).astype(jnp.bfloat16)
    back = jnp.dot(cotangent, flattened_up.T, preferred_element_type=jnp.float32)
    adapted_grad = (back * gain).astype(jnp.bfloat16)
    grad_base = jnp.dot(cotangent, frozen_up_weight.T, preferred_element_type=jnp.float32)
    grad_tokens = (grad_base + jnp.dot(adapted_grad, flattened_down, preferred_element_type=jnp.float32)).astype(jnp.bfloat16)
    grad_up = jnp.dot(adapted.T, cotangent, preferred_element_type=jnp.float32).reshape(TENANT_COUNT, ADAPTER_RANK, HIDDEN_UNITS)
    grad_down = jnp.dot(adapted_grad.T, tokens, preferred_element_type=jnp.float32).reshape(TENANT_COUNT, ADAPTER_RANK, MODEL_WIDTH)
    return hidden_out, grad_tokens, grad_down, grad_up
```

```python
import jax
import jax.numpy as jnp
from jax import lax
from jax.sharding import PartitionSpec as P

BLOCK = 64


alpha_scale = 32.0

BF16 = jnp.bfloat16
F32 = jnp.float32


def nt(a, b):
    return lax.dot_general(a, b, (((1,), (1,)), ((), ())), preferred_element_type=F32)


def tn(a, b):
    return lax.dot_general(a, b, (((0,), (0,)), ((), ())), preferred_element_type=F32)


def fetch_adapter(adapter, tenant_n, dp_n):
    share = adapter.shape[1] // dp_n
    mine = lax.dynamic_slice_in_dim(adapter, lax.axis_index("dp") * share, share, axis=1)
    part = lax.all_to_all(mine, "tenant", split_axis=2, concat_axis=0, tiled=True)
    return lax.all_gather(part, "dp", axis=1, tiled=True)


def reduce_fsdp(x, fsdp_n):
    rows = x.shape[0]
    got = lax.all_to_all(
        x.astype(BF16).reshape(fsdp_n, rows // fsdp_n, x.shape[1]), "fsdp", 0, 0, tiled=True
    )
    total = jnp.sum(got.astype(F32), axis=0).astype(BF16)
    return lax.all_gather(total, "fsdp", axis=0, tiled=True).astype(F32)


def make_shards(mesh):
    tenant_n, fsdp_n, dp_n = mesh.shape["tenant"], mesh.shape["fsdp"], mesh.shape["dp"]

    def shards(tokens, block_tenant_index, ranks, frozen_up_weight, tenant_down_adapters,
               tenant_up_adapters, cotangent):
        rows, local_d = tokens.shape
        local_f = cotangent.shape[1]
        tenants = ranks.shape[0]
        rank = tenant_down_adapters.shape[1]
        depth = frozen_up_weight.shape[0]
        blocks = fsdp_n * dp_n

        first = max(128, (depth * 3 // 5) // 128 * 128) if depth > 128 else depth
        cuts = [(0, first)] + ([(first, depth)] if first < depth else [])
        weights = [
            lax.all_gather(frozen_up_weight[a:b], ("fsdp", "dp"), axis=0, tiled=True)
            for a, b in cuts
        ]
        up = fetch_adapter(tenant_up_adapters, tenant_n, dp_n).reshape(tenants * rank, local_f)
        down = fetch_adapter(tenant_down_adapters, tenant_n, dp_n).reshape(tenants * rank, local_d)

        onehot = (block_tenant_index[:, None] == jnp.arange(tenants, dtype=jnp.int32)[None, :])
        sel = onehot.astype(F32)[:, None, :, None]
        own_rank = jnp.sum(jnp.where(onehot, ranks[None, :], 0), axis=1)
        keep = jnp.arange(rank, dtype=jnp.int32)[None, :] < own_rank[:, None]
        gain = jnp.where(keep, (alpha_scale / own_rank.astype(F32))[:, None], F32(0.0))

        def compact(full):
            full = full.reshape(rows // BLOCK, BLOCK, tenants, rank)
            return jnp.sum(full * sel, axis=2)

        both = jnp.concatenate([compact(nt(tokens, down)), compact(nt(cotangent, up))], axis=2)
        both = lax.psum(both, "tenant")

        def spread(values):
            scaled = (values * gain[:, None, :]).astype(BF16)
            return (scaled[:, :, None, :] * sel.astype(BF16)).reshape(rows, tenants * rank)

        adapted = spread(both[:, :, :rank])
        adapted_grad = spread(both[:, :, rank:])

        terms = jnp.concatenate([tn(adapted, cotangent), tn(adapted_grad, tokens)], axis=1)
        terms = lax.psum_scatter(terms, "dp", scatter_dimension=0, tiled=True)
        grads = reduce_fsdp(terms, fsdp_n)
        grad_up = grads[:, :local_f].reshape(tenants // dp_n, rank, local_f)
        grad_down = grads[:, local_f:].reshape(tenants // dp_n, rank, local_d)

        whole = lax.all_gather(tokens, "tenant", axis=1, tiled=True)
        whole3 = whole.reshape(rows, blocks, depth)
        hidden = jnp.dot(adapted, up, preferred_element_type=F32)
        pieces = []
        for (a, b), weight in zip(cuts, weights):
            back = nt(cotangent, weight).astype(BF16)
            n = b - a
            got = lax.all_to_all(
                back.reshape(rows, tenant_n, blocks * n // tenant_n).transpose(1, 0, 2),
                "tenant", 0, 0, tiled=True,
            )
            pieces.append(jnp.sum(got.astype(F32), axis=0).reshape(rows, blocks // tenant_n, n))
            hidden = hidden + jnp.dot(
                whole3[:, :, a:b].reshape(rows, blocks * n), weight, preferred_element_type=F32
            )
        hidden_out = hidden.astype(BF16)
        grad_base = jnp.concatenate(pieces, axis=2).reshape(rows, local_d)
        grad_tokens = (
            grad_base + jnp.dot(adapted_grad, down, preferred_element_type=F32)
        ).astype(BF16)
        return (hidden_out, grad_tokens, grad_down, grad_up)

    return shards


def solution(mesh):
    return jax.shard_map(
        make_shards(mesh),
        mesh=mesh,
        in_specs=(
            P(("fsdp", "dp"), "tenant"),
            P(("fsdp", "dp")),
            P(),
            P(("fsdp", "dp"), "tenant"),
            P("tenant", None, None),
            P("tenant", None, None),
            P(("fsdp", "dp"), "tenant"),
        ),
        out_specs=(
            P(("fsdp", "dp"), "tenant"),
            P(("fsdp", "dp"), "tenant"),
            P("dp", None, "tenant"),
            P("dp", None, "tenant"),
        ),
        check_vma=False,
    )
```

```python
import math

import jax
import jax.numpy as jnp
from jax import lax
from jax.sharding import PartitionSpec as P

BLOCK = 64


alpha_scale = 32.0

BF16 = jnp.bfloat16
F32 = jnp.float32


def nt(a, b):
    return lax.dot_general(a, b, (((1,), (1,)), ((), ())), preferred_element_type=F32)


def tn(a, b):
    return lax.dot_general(a, b, (((0,), (0,)), ((), ())), preferred_element_type=F32)


def shift(x, axis, n, step):
    return lax.ppermute(x, axis, [(i, (i + step) % n) for i in range(n)])


def put(buffer, value, index):
    return lax.dynamic_update_index_in_dim(buffer, value, index, 0)


def gather_lead(x, axis, n):
    me = lax.axis_index(axis)
    out = put(jnp.zeros((n,) + x.shape, x.dtype), x, me)
    for step in range(1, n):
        out = put(out, shift(x, axis, n, step), (me - step + n) % n)
    return out


def exchange(pick, axis, n):
    me = lax.axis_index(axis)
    out = [(me, pick(me))]
    for step in range(1, n):
        out.append(((me - step + n) % n, shift(pick((me + step) % n), axis, n, step)))
    return out


def ring_order(n):
    side = math.isqrt(n)
    if side * side != n:
        return list(range(n))
    order = []
    for row in range(side):
        cells = [row * side + col for col in range(side)]
        order += cells[::-1] if row % 2 else cells
    return order


def ring_blocks(x, axis, n):
    order = jnp.array(ring_order(n), jnp.int32)
    place = [0] * n
    for spot, device in enumerate(ring_order(n)):
        place[device] = spot
    me = jnp.array(place, jnp.int32)[lax.axis_index(axis)]
    right = [(ring_order(n)[i], ring_order(n)[(i + 1) % n]) for i in range(n)]
    left = [(b, a) for a, b in right]
    out = [(lax.axis_index(axis), x)]
    ahead = behind = x
    for step in range(1, n // 2 + 1):
        if 2 * step == n and n > 2:
            half = x.shape[0] // 2
            top = lax.ppermute(ahead[:half], axis, right)
            low = lax.ppermute(behind[half:], axis, left)
            out.append((order[(me + step) % n], jnp.concatenate([top, low], axis=0)))
            continue
        ahead = lax.ppermute(ahead, axis, right)
        out.append((order[(me - step + n) % n], ahead))
        if 2 * step < n:
            behind = lax.ppermute(behind, axis, left)
            out.append((order[(me + step) % n], behind))
    return out


def fetch_adapter(adapter, tenant_n, dp_n):
    own, rank, width = adapter.shape
    share, local = rank // dp_n, width // tenant_n
    mine = lax.dynamic_slice_in_dim(adapter, lax.axis_index("dp") * share, share, axis=1)
    out = jnp.zeros((tenant_n, own, share, local), adapter.dtype)
    for source, piece in exchange(
        lambda t: lax.dynamic_slice_in_dim(mine, t * local, local, axis=2), "tenant", tenant_n
    ):
        out = put(out, piece, source)
    both = gather_lead(out, "dp", dp_n)
    return both.transpose(1, 2, 0, 3, 4).reshape(tenant_n * own * rank, local)


def reduce_fsdp(x, n):
    rows = x.shape[0] // n
    small = x.astype(BF16)
    total = jnp.zeros((rows, x.shape[1]), F32)
    for _, piece in exchange(
        lambda i: lax.dynamic_slice_in_dim(small, i * rows, rows, axis=0), "fsdp", n
    ):
        total = total + piece.astype(F32)
    return gather_lead(total.astype(BF16), "fsdp", n).reshape(x.shape).astype(F32)


def reduce_dp(x, n):
    rows = x.shape[0] // n
    total = jnp.zeros((rows, x.shape[1]), F32)
    for _, piece in exchange(
        lambda i: lax.dynamic_slice_in_dim(x, i * rows, rows, axis=0), "dp", n
    ):
        total = total + piece
    return total


def make_shards(mesh):
    tenant_n, fsdp_n, dp_n = mesh.shape["tenant"], mesh.shape["fsdp"], mesh.shape["dp"]

    def shards(tokens, block_tenant_index, ranks, frozen_up_weight, tenant_down_adapters,
               tenant_up_adapters, cotangent):
        rows, local_d = tokens.shape
        local_f = cotangent.shape[1]
        tenants = ranks.shape[0]
        rank = tenant_down_adapters.shape[1]
        depth = frozen_up_weight.shape[0]
        blocks = fsdp_n * dp_n
        core = lax.axis_index("dp")

        with jax.named_scope("weight"):
            near = ring_blocks(frozen_up_weight, "fsdp", fsdp_n)
            weights = []
            for source, block in near:
                weights.append((source * dp_n + core, block))
                for step in range(1, dp_n):
                    other = (core - step + dp_n) % dp_n
                    weights.append((source * dp_n + other, shift(block, "dp", dp_n, step)))

        with jax.named_scope("adapters"):
            down = fetch_adapter(tenant_down_adapters, tenant_n, dp_n)
            up = fetch_adapter(tenant_up_adapters, tenant_n, dp_n)

        with jax.named_scope("features"):
            mine = tokens.reshape(rows, local_d // depth, depth).transpose(1, 0, 2)
            whole = gather_lead(mine, "tenant", tenant_n).reshape(blocks, rows, depth)

        onehot = (block_tenant_index[:, None] == jnp.arange(tenants, dtype=jnp.int32)[None, :])
        sel = onehot.astype(F32)[:, None, :, None]
        own_rank = jnp.sum(jnp.where(onehot, ranks[None, :], 0), axis=1)
        keep = jnp.arange(rank, dtype=jnp.int32)[None, :] < own_rank[:, None]
        gain = jnp.where(keep, (alpha_scale / own_rank.astype(F32))[:, None], F32(0.0))

        def compact(full):
            full = full.reshape(rows // BLOCK, BLOCK, tenants, rank)
            return jnp.sum(full * sel, axis=2)

        with jax.named_scope("sums"):
            both = jnp.concatenate([compact(nt(tokens, down)), compact(nt(cotangent, up))], axis=2)
            both = jnp.sum(gather_lead(both, "tenant", tenant_n), axis=0)

        def spread(values):
            scaled = (values * gain[:, None, :]).astype(BF16)
            return (scaled[:, :, None, :] * sel.astype(BF16)).reshape(rows, tenants * rank)

        adapted = spread(both[:, :, :rank])
        adapted_grad = spread(both[:, :, rank:])

        with jax.named_scope("grads"):
            terms = jnp.concatenate([tn(adapted, cotangent), tn(adapted_grad, tokens)], axis=1)
            grads = reduce_fsdp(reduce_dp(terms, dp_n), fsdp_n)
        grad_up = grads[:, :local_f].reshape(tenants // dp_n, rank, local_f)
        grad_down = grads[:, local_f:].reshape(tenants // dp_n, rank, local_d)

        hidden = jnp.dot(adapted, up, preferred_element_type=F32)
        back = jnp.zeros((blocks, rows, depth), BF16)
        for index, weight in weights:
            back = put(back, nt(cotangent, weight).astype(BF16), index)
            part = lax.dynamic_index_in_dim(whole, index, 0, keepdims=False)
            hidden = hidden + jnp.dot(part, weight, preferred_element_type=F32)
        hidden_out = hidden.astype(BF16)
        with jax.named_scope("input_grad"):
            share = blocks // tenant_n
            grad_base = jnp.zeros((share, rows, depth), F32)
            for _, piece in exchange(
                lambda t: lax.dynamic_slice_in_dim(back, t * share, share, axis=0),
                "tenant", tenant_n,
            ):
                grad_base = grad_base + piece.astype(F32)
        grad_tokens = (
            grad_base.transpose(1, 0, 2).reshape(rows, local_d)
            + jnp.dot(adapted_grad, down, preferred_element_type=F32)
        ).astype(BF16)
        return (hidden_out, grad_tokens, grad_down, grad_up)

    return shards


def solution(mesh):
    return jax.shard_map(
        make_shards(mesh),
        mesh=mesh,
        in_specs=(
            P(("fsdp", "dp"), "tenant"),
            P(("fsdp", "dp")),
            P(),
            P(("fsdp", "dp"), "tenant"),
            P("tenant", None, None),
            P("tenant", None, None),
            P(("fsdp", "dp"), "tenant"),
        ),
        out_specs=(
            P(("fsdp", "dp"), "tenant"),
            P(("fsdp", "dp"), "tenant"),
            P("dp", None, "tenant"),
            P("dp", None, "tenant"),
        ),
        check_vma=False,
    )
```

```python
import math

import jax
import jax.numpy as jnp
from jax import lax
from jax.sharding import PartitionSpec as P

BLOCK = 64


alpha_scale = 32.0

BF16 = jnp.bfloat16
F32 = jnp.float32


def nt(a, b):
    return lax.dot_general(a, b, (((1,), (1,)), ((), ())), preferred_element_type=F32)


def tn(a, b):
    return lax.dot_general(a, b, (((0,), (0,)), ((), ())), preferred_element_type=F32)


def shift(x, axis, n, step):
    return lax.ppermute(x, axis, [(i, (i + step) % n) for i in range(n)])


def put(buffer, value, index):
    return lax.dynamic_update_index_in_dim(buffer, value, index, 0)


def gather_lead(x, axis, n):
    me = lax.axis_index(axis)
    out = put(jnp.zeros((n,) + x.shape, x.dtype), x, me)
    for step in range(1, n):
        out = put(out, shift(x, axis, n, step), (me - step + n) % n)
    return out


def exchange(pick, axis, n):
    me = lax.axis_index(axis)
    out = [(me, pick(me))]
    for step in range(1, n):
        out.append(((me - step + n) % n, shift(pick((me + step) % n), axis, n, step)))
    return out


def ring_order(n):
    side = math.isqrt(n)
    if side * side != n:
        return list(range(n))
    order = []
    for row in range(side):
        cells = [row * side + col for col in range(side)]
        order += cells[::-1] if row % 2 else cells
    return order


def ring_blocks(x, axis, n):
    order = jnp.array(ring_order(n), jnp.int32)
    place = [0] * n
    for spot, device in enumerate(ring_order(n)):
        place[device] = spot
    me = jnp.array(place, jnp.int32)[lax.axis_index(axis)]
    right = [(ring_order(n)[i], ring_order(n)[(i + 1) % n]) for i in range(n)]
    left = [(b, a) for a, b in right]
    out = [(lax.axis_index(axis), x)]
    half = x.shape[0] // 2
    ahead = behind = (x[:half], x[half:])
    relayed = ()
    for step in range(1, n // 2 + 1):
        if 2 * step == n and n > 2:
            relayed = (ahead[0], behind[1])
            halves = (lax.ppermute(ahead[0], axis, right), lax.ppermute(behind[1], axis, left))
            out.append((order[(me + step) % n], jnp.concatenate(halves, axis=0)))
            continue
        top = lax.ppermute(ahead[0], axis, right)
        ahead = (top, lax.ppermute(ahead[1], axis, right))
        out.append((order[(me - step + n) % n], jnp.concatenate(ahead, axis=0)))
        if 2 * step < n:
            low = lax.ppermute(behind[1], axis, left)
            behind = (lax.ppermute(behind[0], axis, left), low)
            out.append((order[(me + step) % n], jnp.concatenate(behind, axis=0)))
    return out, relayed


def fetch_adapter(adapter, tenant_n, dp_n):
    own, rank, width = adapter.shape
    share, local = rank // dp_n, width // tenant_n
    mine = lax.dynamic_slice_in_dim(adapter, lax.axis_index("dp") * share, share, axis=1)
    out = jnp.zeros((tenant_n, own, share, local), adapter.dtype)
    for source, piece in exchange(
        lambda t: lax.dynamic_slice_in_dim(mine, t * local, local, axis=2), "tenant", tenant_n
    ):
        out = put(out, piece, source)
    both = gather_lead(out, "dp", dp_n)
    return both.transpose(1, 2, 0, 3, 4).reshape(tenant_n * own * rank, local)


def reduce_fsdp(x, n):
    rows = x.shape[0] // n
    small = x.astype(BF16)
    total = jnp.zeros((rows, x.shape[1]), F32)
    for _, piece in exchange(
        lambda i: lax.dynamic_slice_in_dim(small, i * rows, rows, axis=0), "fsdp", n
    ):
        total = total + piece.astype(F32)
    return gather_lead(total.astype(BF16), "fsdp", n).reshape(x.shape).astype(F32)


def reduce_dp(x, n):
    rows = x.shape[0] // n
    total = jnp.zeros((rows, x.shape[1]), F32)
    for _, piece in exchange(
        lambda i: lax.dynamic_slice_in_dim(x, i * rows, rows, axis=0), "dp", n
    ):
        total = total + piece
    return total


def make_shards(mesh):
    tenant_n, fsdp_n, dp_n = mesh.shape["tenant"], mesh.shape["fsdp"], mesh.shape["dp"]

    def shards(tokens, block_tenant_index, ranks, frozen_up_weight, tenant_down_adapters,
               tenant_up_adapters, cotangent):
        rows, local_d = tokens.shape
        local_f = cotangent.shape[1]
        tenants = ranks.shape[0]
        rank = tenant_down_adapters.shape[1]
        depth = frozen_up_weight.shape[0]
        blocks = fsdp_n * dp_n
        core = lax.axis_index("dp")

        with jax.named_scope("weight"):
            near, relayed = ring_blocks(frozen_up_weight, "fsdp", fsdp_n)
            weights = []
            for source, block in near:
                weights.append((source * dp_n + core, block))
                for step in range(1, dp_n):
                    other = (core - step + dp_n) % dp_n
                    weights.append((source * dp_n + other, shift(block, "dp", dp_n, step)))

        with jax.named_scope("adapters"):
            down = fetch_adapter(tenant_down_adapters, tenant_n, dp_n)
            up = fetch_adapter(tenant_up_adapters, tenant_n, dp_n)

        onehot = (block_tenant_index[:, None] == jnp.arange(tenants, dtype=jnp.int32)[None, :])
        sel = onehot.astype(F32)[:, None, :, None]
        own_rank = jnp.sum(jnp.where(onehot, ranks[None, :], 0), axis=1)
        keep = jnp.arange(rank, dtype=jnp.int32)[None, :] < own_rank[:, None]
        gain = jnp.where(keep, (alpha_scale / own_rank.astype(F32))[:, None], F32(0.0))

        def compact(full):
            full = full.reshape(rows // BLOCK, BLOCK, tenants, rank)
            return jnp.sum(full * sel, axis=2)

        with jax.named_scope("sums"):
            both = jnp.concatenate([compact(nt(tokens, down)), compact(nt(cotangent, up))], axis=2)
            both = jnp.sum(gather_lead(both, "tenant", tenant_n), axis=0)

        with jax.named_scope("features"):
            mine = tokens.reshape(rows, local_d // depth, depth).transpose(1, 0, 2)
            mine, both = lax.optimization_barrier((mine, both) + relayed)[:2]
            whole = gather_lead(mine, "tenant", tenant_n).reshape(blocks, rows, depth)

        def spread(values):
            scaled = (values * gain[:, None, :]).astype(BF16)
            return (scaled[:, :, None, :] * sel.astype(BF16)).reshape(rows, tenants * rank)

        adapted = spread(both[:, :, :rank])
        adapted_grad = spread(both[:, :, rank:])

        with jax.named_scope("grads"):
            terms = jnp.concatenate([tn(adapted, cotangent), tn(adapted_grad, tokens)], axis=1)
            grads = reduce_fsdp(reduce_dp(terms, dp_n), fsdp_n)
        grad_up = grads[:, :local_f].reshape(tenants // dp_n, rank, local_f)
        grad_down = grads[:, local_f:].reshape(tenants // dp_n, rank, local_d)

        hidden = jnp.dot(adapted, up, preferred_element_type=F32)
        back = jnp.zeros((blocks, rows, depth), BF16)
        for index, weight in weights:
            back = put(back, nt(cotangent, weight).astype(BF16), index)
            part = lax.dynamic_index_in_dim(whole, index, 0, keepdims=False)
            hidden = hidden + jnp.dot(part, weight, preferred_element_type=F32)
        hidden_out = hidden.astype(BF16)
        with jax.named_scope("input_grad"):
            share = blocks // tenant_n
            grad_base = jnp.zeros((share, rows, depth), F32)
            for _, piece in exchange(
                lambda t: lax.dynamic_slice_in_dim(back, t * share, share, axis=0),
                "tenant", tenant_n,
            ):
                grad_base = grad_base + piece.astype(F32)
        grad_tokens = (
            grad_base.transpose(1, 0, 2).reshape(rows, local_d)
            + jnp.dot(adapted_grad, down, preferred_element_type=F32)
        ).astype(BF16)
        return (hidden_out, grad_tokens, grad_down, grad_up)

    return shards


def solution(mesh):
    return jax.shard_map(
        make_shards(mesh),
        mesh=mesh,
        in_specs=(
            P(("fsdp", "dp"), "tenant"),
            P(("fsdp", "dp")),
            P(),
            P(("fsdp", "dp"), "tenant"),
            P("tenant", None, None),
            P("tenant", None, None),
            P(("fsdp", "dp"), "tenant"),
        ),
        out_specs=(
            P(("fsdp", "dp"), "tenant"),
            P(("fsdp", "dp"), "tenant"),
            P("dp", None, "tenant"),
            P("dp", None, "tenant"),
        ),
        check_vma=False,
    )
```
